32 devices in a mesh: rep: 8 (over z, core), fsdp: 4 (over y, x).
Axes of the slice: x: 2, y: 2, z: 4, core: 2. Of those that a mesh axis runs over, the one named last changes fastest.
Arguments:
- tokens: bfloat16 [8, 512, 8192], P('rep', 'fsdp'), may hold values from -6 to 6
- norm_gain: bfloat16 [8192], replicated, may hold values from 0.25 to 1.75
- inner_weight: bfloat16 [8, 8192, 512], P('rep', 'fsdp'), may hold values from -0.0625 to 0.0625
- cotangent: bfloat16 [8, 512, 512], P('rep', 'fsdp'), may hold values from -6 to 6
- fragment: bfloat16 [8, 8192, 512], P('rep', 'fsdp'), may hold values from -6 to 6
- outer_param: float32 [8192, 512], P('fsdp'), may hold values from -6 to 6
- momentum: bfloat16 [8192, 512], P('fsdp'), may hold values from -3 to 3
- lag: int32 [8], P('rep'), may hold values from 0 to 7, as said below
- threshold: int32 [1], replicated, may hold values from 1 to 6
Outputs:
- inner_grad: bfloat16 [8, 8192, 512], P('rep', 'fsdp')
- mixed: bfloat16 [8, 8192, 512], P('rep', 'fsdp')
- new_momentum: bfloat16 [8192, 512], P('fsdp')
The draws below stay inside these ranges and needn't reach their ends.
Inputs may be any that keep to these rules, and one draw needn't show every extreme that they name: At least one replica has lag 0.
All inputs are finite; a program needn't handle non-finite values.
Results may differ from the reference program's by a relative error of at most 0.006.
Values may be sent and summed in bfloat16 or wider, within the bound.
No kernel may reach another device: no remote copies, remote signals or barrier semaphores. Data moves between devices by JAX's collectives and lax.ppermute only.
A program may use at most 64 MiB of HBM per device.

```python
import math
import jax
import jax.numpy as jnp
from jax import lax

D = 8192
KVW = 512
TOKF = 512
REPLICAS = 8


def draw_lag(key, part):
    first, second = jax.random.split(jax.random.fold_in(key, 11))
    values = jax.random.randint(first, (REPLICAS,), 0, 8, dtype=jnp.int32)
    spot = jax.random.randint(second, (), 0, REPLICAS, dtype=jnp.int32)
    return jnp.where(jnp.arange(REPLICAS, dtype=jnp.int32) == spot, 0, values).astype(jnp.int32)


def shard_levels(rng, shape, shards, least, largest):
    def one(dim, shards_of):
        draws = jax.random.uniform(jax.random.fold_in(jax.random.fold_in(rng, 6), dim), (shards_of,), jnp.float32, least / len(shards), largest / len(shards))
        return jnp.repeat(jnp.exp(draws), shape[dim] // shards_of).reshape((-1,) + (1,) * (len(shape) - dim - 1))

    factor_of = one(*shards[0])
    for cut in shards[1:]:
        factor_of = factor_of * one(*cut)
    return factor_of


def normal_values(own_key, dims, width, reach, shards=(), kind=jnp.bfloat16):
    array = jax.random.normal(own_key, dims, jnp.float32) * width
    if len(shards) > 0:
        array = shard_levels(own_key, dims, shards, -0.22, 0.18) * array
    return jnp.clip(array, min=-reach, max=reach).astype(kind)


def setup_inputs(seed: int = 0) -> dict:
    splits = jax.random.split(jax.random.key(seed), 10)
    tokens = normal_values(splits[0], (REPLICAS, TOKF, D), 1.0, 6.0, ((0, 8), (1, 4)))
    norm_gain = jnp.clip(1.0 + 0.15 * jax.random.normal(splits[1], (D,), jnp.float32), 0.25, 1.75).astype(jnp.bfloat16)
    inner_weight = normal_values(splits[2], (REPLICAS, D, KVW), D ** -0.5, 0.0625, ((0, 8), (1, 4)))
    cotangent = normal_values(splits[3], (REPLICAS, TOKF, KVW), 1.0, 6.0, ((0, 8), (1, 4)))
    fragment = normal_values(splits[4], (REPLICAS, D, KVW), 1.0, 6.0, ((0, 8), (1, 4)))
    outer_param = normal_values(splits[5], (D, KVW), 1.0, 6.0, ((0, 4),), jnp.float32)
    momentum = normal_values(splits[6], (D, KVW), 0.5, 3.0, ((0, 4),))
    lag = draw_lag(jax.random.fold_in(splits[9], 71), 0)
    threshold = jax.random.randint(splits[8], (1,), 1, 7).astype(jnp.int32)
    return dict(tokens=tokens, norm_gain=norm_gain, inner_weight=inner_weight, cotangent=cotangent, fragment=fragment, outer_param=outer_param, momentum=momentum, lag=lag, threshold=threshold)


EPS = 1e-05
MU = 0.9
OUTER_LR = 0.7
ALPHA = 0.5

def inner_step(norm_gain, operands):
    hidden, weight, cotangent = operands
    values = hidden.astype(jnp.float32)
    normed = (values * lax.rsqrt(lax.optimization_barrier(jnp.mean(values * values, axis=1, keepdims=True)) + EPS) * norm_gain.astype(jnp.float32)).astype(jnp.bfloat16)
    key_rows = jnp.dot(normed, weight, preferred_element_type=jnp.float32)
    sigmoid_keys = jax.nn.sigmoid(key_rows)
    dkeys = (cotangent.astype(jnp.float32) * sigmoid_keys * (1.0 + key_rows * (1.0 - sigmoid_keys))).astype(jnp.bfloat16)
    gradient = lax.dot_general(normed, dkeys, (((0,), (0,)), ((), ())), preferred_element_type=jnp.float32)
    return (gradient * (1.0 / math.sqrt(hidden.shape[0]))).astype(jnp.bfloat16)

def reference(tokens, norm_gain, inner_weight, cotangent, fragment, outer_param, momentum, lag, threshold):
    inner_grad = lax.map(lambda operands: inner_step(norm_gain, operands), (tokens, inner_weight, cotangent))
    included = (lag <= threshold[0]).astype(jnp.float32)
    count = jnp.sum(included)
    scale = 1.0 / count

    def accumulate(total, operands):
        replica_frag, flag = operands
        return (total + flag * (outer_param - replica_frag.astype(jnp.float32)), None)
    total, _ = lax.scan(accumulate, jnp.zeros(outer_param.shape, jnp.float32), (fragment, included))
    average = total * scale
    moment = MU * momentum.astype(jnp.float32) + average
    new_outer = outer_param - OUTER_LR * (average + MU * moment)
    mixed = (ALPHA * fragment.astype(jnp.float32) + (1.0 - ALPHA) * new_outer[None]).astype(jnp.bfloat16)
    return (inner_grad, mixed, moment.astype(jnp.bfloat16))
```

```python
import functools
import math

import jax
import jax.numpy as jnp
from jax import lax
from jax.experimental import pallas as pl
from jax.experimental.pallas import tpu as pltpu
from jax.sharding import PartitionSpec as P

EPS = 1e-05
MU = 0.9
OUTER_LR = 0.7
ALPHA = 0.5
CHUNKS = 4

F32 = jnp.float32
BF16 = jnp.bfloat16


def norm_kernel(order_ref, tokens_ref, gain_ref, *out_refs):
    values = tokens_ref[...].astype(F32)
    scale = lax.rsqrt(jnp.mean(values * values, axis=1, keepdims=True) + EPS)
    width = out_refs[0].shape[1]
    for slot, out_ref in enumerate(out_refs):
        columns = pl.ds(pl.multiple_of(order_ref[slot] * width, width), width)
        block = tokens_ref[:, columns].astype(F32)
        gain = gain_ref[:, columns].astype(F32)
        out_ref[...] = (block * scale * gain).astype(BF16)


def normed_blocks(tokens, norm_gain, order):
    rows, features = tokens.shape
    slots = order.shape[0]
    tile = math.gcd(rows, 32)
    return pl.pallas_call(
        norm_kernel,
        grid_spec=pltpu.PrefetchScalarGridSpec(
            num_scalar_prefetch=1,
            grid=(rows // tile,),
            in_specs=[
                pl.BlockSpec((tile, features), lambda i, o: (i, 0)),
                pl.BlockSpec((1, features), lambda i, o: (0, 0)),
            ],
            out_specs=[pl.BlockSpec((tile, features // slots), lambda i, o: (i, 0))] * slots,
        ),
        out_shape=[jax.ShapeDtypeStruct((rows, features // slots), BF16)] * slots,
        cost_estimate=pl.CostEstimate(
            flops=6 * rows * features, bytes_accessed=4 * rows * features, transcendentals=rows
        ),
        name="norm_split",
    )(order, tokens, norm_gain.reshape(1, features))


def grad_kernel(scale, count, *refs):
    out_ref = refs[-1]
    total = None
    for n_ref, d_ref in zip(refs[:count], refs[count : 2 * count]):
        part = lax.dot_general(
            n_ref[...], d_ref[...], (((0,), (0,)), ((), ())), preferred_element_type=F32
        )
        total = part if total is None else total + part
    out_ref[0] = (total * scale).astype(BF16)


def gradient_of(normed, dkeys):
    rows, features = normed[0].shape
    width = dkeys[0].shape[1]
    count = len(normed)
    tile = math.gcd(features, 512)
    tokens = rows * count
    return pl.pallas_call(
        functools.partial(grad_kernel, 1.0 / math.sqrt(tokens), count),
        grid=(features // tile,),
        in_specs=[pl.BlockSpec((rows, tile), lambda i: (0, i))] * count
        + [pl.BlockSpec((rows, width), lambda i: (0, 0))] * count,
        out_specs=pl.BlockSpec((1, tile, width), lambda i: (0, i, 0)),
        out_shape=jax.ShapeDtypeStruct((1, features, width), BF16),
        cost_estimate=pl.CostEstimate(
            flops=2 * tokens * features * width,
            bytes_accessed=2 * (tokens * (features + width) + features * width),
            transcendentals=0,
        ),
        name="key_grad",
    )(*normed, *dkeys)


def inner_part(tokens, norm_gain, inner_weight, cotangent):
    size = lax.axis_size("fsdp")
    me = lax.axis_index("fsdp")
    if size & (size - 1) == 0:
        to = [[i ^ s for i in range(size)] for s in range(size)]
        order = jnp.bitwise_xor(me, jnp.arange(size, dtype=jnp.int32))
    else:
        to = [[(i + s) % size for i in range(size)] for s in range(size)]
        order = lax.rem(me + jnp.arange(size, dtype=jnp.int32), size)

    def send(value, slot):
        return lax.ppermute(value, "fsdp", [(i, to[slot][i]) for i in range(size)])

    def send_back(value, slot):
        return lax.ppermute(value, "fsdp", [(to[slot][i], i) for i in range(size)])

    weight = inner_weight[0]
    blocks = normed_blocks(tokens[0], norm_gain, order)
    normed = [blocks[0]] + [send(blocks[s], s) for s in range(1, size)]
    keys = jnp.dot(normed[0], weight, preferred_element_type=F32)
    for s in range(1, size):
        partial_keys = jnp.dot(normed[s], weight, preferred_element_type=F32).astype(BF16)
        keys = keys + send_back(partial_keys, s).astype(F32)
    sigmoid_keys = jax.nn.sigmoid(keys)
    own = (cotangent[0].astype(F32) * sigmoid_keys * (1.0 + keys * (1.0 - sigmoid_keys))).astype(
        BF16
    )
    dkeys = [own] + [send(own, s) for s in range(1, size)]
    return gradient_of(normed, dkeys)


def line_sum(value, rounded_add):
    chips = lax.axis_size("rep") // 2
    chip = lax.axis_index("rep") // 2

    def hop(x, moves):
        return lax.ppermute(
            x, "rep", [(2 * a + core, 2 * b + core) for a, b in moves for core in range(2)]
        )

    half = chips // 2
    if chips == 1:
        return value
    for s in range(half - 1):
        value = rounded_add(value, hop(value, [(s, s + 1), (chips - 1 - s, chips - 2 - s)]))
    value = rounded_add(value, hop(value, [(half - 1, half), (half, half - 1)]))
    for s in reversed(range(half - 1)):
        passed = hop(value, [(s + 1, s), (chips - 2 - s, chips - 1 - s)])
        value = jnp.where((chip == s) | (chip == chips - 1 - s), passed, value)
    return value


def rounded(x):
    return lax.reduce_precision(x, 8, 7).astype(BF16)


def final_kernel(scalars_ref, count_ref, own_ref, other_ref, outer_ref, momentum_ref, frag_ref, *refs):
    mixed_ref, moment_ref = refs[-2:]
    scale = 1.0 / count_ref[0]
    total = jnp.where(pl.program_id(0) == 0, own_ref[...].astype(F32), other_ref[...].astype(F32))
    average = total * scale
    outer = outer_ref[...]
    moment = MU * momentum_ref[...].astype(F32) + average
    new_outer = outer - OUTER_LR * (average + MU * moment)
    mixed_ref[0] = (ALPHA * frag_ref[0].astype(F32) + (1.0 - ALPHA) * new_outer).astype(BF16)
    moment_ref[...] = moment.astype(BF16)


def finish_chunk(chunk, chunks, core, count, own, other, outer, momentum, fragment, carried):
    rows, width = outer.shape
    tile = own.shape[0]

    def at(g, s):
        return (lax.rem(s[0] + g, 2) * chunks + chunk, 0)

    def at3(g, s):
        return (0, lax.rem(s[0] + g, 2) * chunks + chunk, 0)

    flat = pl.BlockSpec((tile, width), at)
    deep = pl.BlockSpec((1, tile, width), at3)
    whole = pl.BlockSpec((tile, width), lambda g, s: (0, 0))
    extra = [pl.BlockSpec(memory_space=pl.ANY)] * len(carried)
    return pl.pallas_call(
        final_kernel,
        grid_spec=pltpu.PrefetchScalarGridSpec(
            num_scalar_prefetch=1,
            grid=(2,),
            in_specs=[pl.BlockSpec(memory_space=pltpu.SMEM), whole, whole, flat, flat, deep] + extra,
            out_specs=[deep, flat],
        ),
        out_shape=[
            jax.ShapeDtypeStruct((1, rows, width), BF16),
            jax.ShapeDtypeStruct((rows, width), BF16),
        ],
        input_output_aliases={7 + k: k for k in range(len(carried))},
        cost_estimate=pl.CostEstimate(
            flops=20 * tile * width, bytes_accessed=32 * tile * width, transcendentals=0
        ),
        name="outer_step",
    )(core, count, own, other, outer, momentum, fragment, *carried)


def fragment_part(fragment, outer_param, momentum, lag, threshold):
    rep = lax.axis_index("rep")
    core = lax.rem(rep, 2)
    pairs = [(r, r ^ 1) for r in range(lax.axis_size("rep"))]
    rows, width = outer_param.shape
    half = rows // 2
    tile = half // CHUNKS

    def across(x):
        return lax.ppermute(x, "rep", pairs)

    frag = fragment[0]
    flag = (lag[0] <= threshold[0]).astype(F32)
    other_flag = (across(lag)[0] <= threshold[0]).astype(F32)
    other_frag = across(lax.dynamic_slice(frag, ((1 - core) * half, 0), (half, width)))

    def chunk_of(x, k):
        return lax.dynamic_slice(x, (core * half + k * tile, 0), (tile, width))

    def add(a, b):
        return rounded(a.astype(F32) + b.astype(F32))

    totals = []
    for k in range(CHUNKS):
        outer_k = chunk_of(outer_param, k)
        mine = flag * (outer_k - chunk_of(frag, k).astype(F32))
        theirs = other_flag * (outer_k - other_frag[k * tile : (k + 1) * tile].astype(F32))
        term = mine + theirs
        if k == 0:
            term = jnp.concatenate([term, jnp.full((16, width), flag + other_flag, F32)])
        total = line_sum(rounded(term), add)
        if k == 0:
            count = total[tile, 0:1].astype(F32)
            total = total[:tile]
        totals.append(total)
    carried = ()
    for k in range(CHUNKS):
        carried = finish_chunk(
            k, CHUNKS, core[None], count, totals[k], across(totals[k]), outer_param, momentum,
            fragment, carried,
        )
    return carried


def shards(
    tokens, norm_gain, inner_weight, cotangent, fragment, outer_param, momentum, lag, threshold
):
    inner_grad = inner_part(tokens, norm_gain, inner_weight, cotangent)
    mixed, new_momentum = fragment_part(fragment, outer_param, momentum, lag, threshold)
    return (inner_grad, mixed, new_momentum)


def solution(mesh):
    placed = (
        P("rep", "fsdp", None),
        P(),
        P("rep", "fsdp", None),
        P("rep", "fsdp", None),
        P("rep", "fsdp", None),
        P("fsdp", None),
        P("fsdp", None),
        P("rep"),
        P(),
    )
    return jax.shard_map(
        shards,
        mesh=mesh,
        in_specs=placed,
        out_specs=(P("rep", "fsdp", None), P("rep", "fsdp", None), P("fsdp", None)),
        check_vma=False,
    )
```

```python
import functools
import math

import jax
import jax.numpy as jnp
from jax import lax
from jax.experimental import pallas as pl
from jax.experimental.pallas import tpu as pltpu
from jax.sharding import PartitionSpec as P


EPS = 1e-05
MU = 0.9
OUTER_LR = 0.7
ALPHA = 0.5
CHUNKS = 2

F32 = jnp.float32
BF16 = jnp.bfloat16


def in_hbm(x):
    return pltpu.with_memory_space_constraint(x, pltpu.HBM)


def norm_kernel(order_ref, tokens_ref, gain_ref, *out_refs):
    lanes = gain_ref.shape[1]
    tile, features = tokens_ref.shape
    squares = jnp.zeros((tile, lanes), F32)
    for g in range(features // lanes):
        block = tokens_ref[:, g * lanes : (g + 1) * lanes].astype(F32)
        squares = squares + block * block
    scale = lax.rsqrt(jnp.sum(squares, axis=1, keepdims=True) * (1.0 / features) + EPS)
    scale = jnp.broadcast_to(scale, (tile, lanes))
    rows = pl.ds(pl.multiple_of(pl.program_id(0) * tile, tile), tile)
    groups = out_refs[0].shape[1] // lanes
    for slot, out_ref in enumerate(out_refs):
        first = pl.multiple_of(order_ref[slot] * groups, groups)
        if groups % 8 == 0:
            gain = gain_ref[pl.ds(first, groups), :].astype(F32)
        else:
            gain = jnp.concatenate([gain_ref[pl.ds(first + g, 1), :] for g in range(groups)])
        for g in range(groups):
            columns = pl.ds(pl.multiple_of((first + g) * lanes, lanes), lanes)
            block = tokens_ref[:, columns].astype(F32)
            out_ref[rows, g * lanes : (g + 1) * lanes] = (block * scale * gain[g : g + 1]).astype(BF16)


def normed_blocks(tokens, norm_gain, order):
    rows, features = tokens.shape
    slots = order.shape[0]
    tile = math.gcd(rows, 32)
    lanes = 128
    gain = norm_gain.reshape(features // lanes, lanes)
    if features // slots // lanes % 8:
        gain = gain.astype(F32)
    return pl.pallas_call(
        norm_kernel,
        grid_spec=pltpu.PrefetchScalarGridSpec(
            num_scalar_prefetch=1,
            grid=(rows // tile,),
            in_specs=[
                pl.BlockSpec((tile, features), lambda i, o: (i, 0)),
                pl.BlockSpec((features // lanes, lanes), lambda i, o: (0, 0)),
            ],
            out_specs=[pl.BlockSpec(memory_space=pltpu.VMEM)] * slots,
        ),
        out_shape=[jax.ShapeDtypeStruct((rows, features // slots), BF16)] * slots,
        cost_estimate=pl.CostEstimate(
            flops=6 * rows * features, bytes_accessed=4 * rows * features, transcendentals=rows
        ),
        compiler_params=pltpu.CompilerParams(vmem_limit_bytes=16 * rows * features),
        name="norm_split",
    )(order, in_hbm(tokens), in_hbm(gain))


def gradient_of(normed, dkeys):
    lhs = jnp.concatenate(normed)
    gradient = lax.dot_general(
        lhs, jnp.concatenate(dkeys), (((0,), (0,)), ((), ())), preferred_element_type=F32
    )
    return (gradient * (1.0 / math.sqrt(lhs.shape[0])))[None].astype(BF16)


def inner_part(tokens, norm_gain, inner_weight, cotangent):
    size = lax.axis_size("fsdp")
    me = lax.axis_index("fsdp")
    if size & (size - 1) == 0:
        to = [[i ^ s for i in range(size)] for s in range(size)]
        order = jnp.bitwise_xor(me, jnp.arange(size, dtype=jnp.int32))
    else:
        to = [[(i + s) % size for i in range(size)] for s in range(size)]
        order = lax.rem(me + jnp.arange(size, dtype=jnp.int32), size)

    def send(value, slot):
        return lax.ppermute(value, "fsdp", [(i, to[slot][i]) for i in range(size)])

    def send_back(value, slot):
        return lax.ppermute(value, "fsdp", [(to[slot][i], i) for i in range(size)])

    weight = inner_weight[0]
    blocks = normed_blocks(tokens[0], norm_gain, order)
    normed = [blocks[0]] + [send(blocks[s], s) for s in range(1, size)]
    keys = jnp.dot(normed[0], weight, preferred_element_type=F32)
    for s in range(1, size):
        partial_keys = jnp.dot(normed[s], weight, preferred_element_type=F32).astype(BF16)
        keys = keys + send_back(partial_keys, s).astype(F32)
    sigmoid_keys = jax.nn.sigmoid(keys)
    slope = sigmoid_keys * (1.0 + keys * (1.0 - sigmoid_keys))
    own = (cotangent[0].astype(F32) * slope).astype(BF16)
    dkeys = [own] + [send(own, s) for s in range(1, size)]
    return gradient_of(normed, dkeys)


def rounded(x):
    return lax.reduce_precision(x, 8, 7).astype(BF16)


def line_sum(term, chips, position, hop):
    half = chips // 2
    for s in range(half - 1):
        term = rounded(term.astype(F32) + hop(term, [(s, s + 1), (chips - 1 - s, chips - 2 - s)]))
    passed = hop(term, [(half - 1, half), (half, half - 1)])
    term = rounded(term.astype(F32) + passed.astype(F32))
    for s in reversed(range(half - 1)):
        passed = hop(term, [(s + 1, s), (chips - 2 - s, chips - 1 - s)])
        term = jnp.where((position == s) | (position == chips - 1 - s), passed, term)
    return term


def outer_kernel(chunk_first, head_ref, *refs):
    totals = refs[:4]
    outer_hbm, momentum_hbm, frag_hbm = refs[4:7]
    mixed_hbm, moment_hbm, outer, momentum, frag, mixed, moment, in_sems, out_sems = refs[-9:]
    strips, strip, _ = outer.shape
    half = outer_hbm.shape[0] // 2
    rep = lax.axis_index("rep")
    core = lax.rem(rep, 2)
    odd = lax.rem(rep // 2, 2)

    def start_row(j):
        side = core if j // 2 == 0 else 1 - core
        place = odd if j % 2 == 0 else 1 - odd
        return pl.multiple_of(side * half + chunk_first + place * strip, strip)

    def loads(j):
        rows = pl.ds(start_row(j), strip)
        return (
            pltpu.make_async_copy(outer_hbm.at[rows], outer.at[j], in_sems.at[j, 0]),
            pltpu.make_async_copy(momentum_hbm.at[rows], momentum.at[j], in_sems.at[j, 1]),
            pltpu.make_async_copy(frag_hbm.at[0, rows], frag.at[j], in_sems.at[j, 2]),
        )

    def stores(j):
        rows = pl.ds(start_row(j), strip)
        return (
            pltpu.make_async_copy(mixed.at[j], mixed_hbm.at[0, rows], out_sems.at[j, 0]),
            pltpu.make_async_copy(moment.at[j], moment_hbm.at[rows], out_sems.at[j, 1]),
        )

    for j in range(strips):
        for copy in loads(j):
            copy.start()
    margin = head_ref.shape[0] - strip
    scale = 1.0 / head_ref[strip:, :].astype(F32)
    for j in range(strips):
        for copy in loads(j):
            copy.wait()

        @pl.loop(0, strip // margin, unroll=True)
        def _(i):
            rows = pl.ds(pl.multiple_of(i * margin, margin), margin)
            average = totals[j][rows].astype(F32) * scale
            value = outer[j, rows]
            new_moment = MU * momentum[j, rows].astype(F32) + average
            new_outer = value - OUTER_LR * (average + MU * new_moment)
            mixed[j, rows] = (ALPHA * frag[j, rows].astype(F32) + (1.0 - ALPHA) * new_outer).astype(BF16)
            moment[j, rows] = new_moment.astype(BF16)

        for copy in stores(j):
            copy.start()
    for j in range(strips):
        for copy in stores(j):
            copy.wait()


def outer_step(chunk_first, strip, head, totals, outer, momentum, fragment, carried):
    rows, width = outer.shape
    strips = len(totals)
    hbm = pl.BlockSpec(memory_space=pltpu.HBM)
    vmem = pl.BlockSpec(memory_space=pltpu.VMEM)
    block = (strips, strip, width)
    return pl.pallas_call(
        functools.partial(outer_kernel, chunk_first),
        in_specs=[vmem] * (1 + strips) + [hbm] * (3 + len(carried)),
        out_specs=[hbm, hbm],
        out_shape=[
            jax.ShapeDtypeStruct((1, rows, width), BF16),
            jax.ShapeDtypeStruct((rows, width), BF16),
        ],
        scratch_shapes=[
            pltpu.VMEM(block, F32),
            pltpu.VMEM(block, BF16),
            pltpu.VMEM(block, BF16),
            pltpu.VMEM(block, BF16),
            pltpu.VMEM(block, BF16),
            pltpu.SemaphoreType.DMA((strips, 3)),
            pltpu.SemaphoreType.DMA((strips, 2)),
        ],
        input_output_aliases={4 + strips + k: k for k in range(len(carried))},
        cost_estimate=pl.CostEstimate(
            flops=20 * strips * strip * width,
            bytes_accessed=14 * strips * strip * width,
            transcendentals=0,
        ),
        compiler_params=pltpu.CompilerParams(vmem_limit_bytes=24 * strips * strip * width),
        name="outer_step",
    )(head, *totals, outer, momentum, fragment, *carried)


def fragment_part(fragment, outer_param, momentum, lag, threshold):
    size = lax.axis_size("rep")
    rep = lax.axis_index("rep")
    core = lax.rem(rep, 2)
    chips = size // 2
    odd = lax.rem(rep // 2, 2)
    rows, width = outer_param.shape
    half = rows // 2
    tile = half // CHUNKS
    part = tile // 2
    margin = 16

    def move(x, pairs):
        return lax.ppermute(x, "rep", pairs)

    def across(x):
        return move(x, [(r, r ^ 1) for r in range(size)])

    def next_chip(x):
        return move(x, [(r, r ^ 2) for r in range(size)])

    frag = fragment[0]
    other_frag = across(frag)
    flag = (lag[0] <= threshold[0]).astype(F32)
    other_flag = (across(lag)[0] <= threshold[0]).astype(F32)

    def term_of(k, which):
        def rows_of(x):
            start = core * half + k * tile + which * part
            return lax.dynamic_slice(x, (start, 0), (part, width))

        outer_k = rows_of(outer_param)
        mine = flag * (outer_k - rows_of(frag).astype(F32))
        theirs = other_flag * (outer_k - rows_of(other_frag).astype(F32))
        term = mine + theirs
        if k == 0:
            return jnp.concatenate([term, jnp.full((margin, width), flag + other_flag, F32)])
        return term

    totals = []
    for k in range(CHUNKS):
        sent, kept = lax.optimization_barrier((rounded(term_of(k, 1 - odd)), term_of(k, odd)))
        passed = next_chip(sent)
        value = rounded(kept + passed.astype(F32))

        def hop(x, moves):
            pairs = [
                (4 * a + r, 4 * b + r) for a, b in moves for r in range(4)
            ]
            return move(x, pairs)

        value = line_sum(value, chips // 2, rep // 4, hop)
        other = next_chip(value)
        far = across(value)
        totals.append((value, other, far, across(other)))
    carried = ()
    for k in range(CHUNKS):
        carried = outer_step(
            k * tile, part, totals[0][0], totals[k], in_hbm(outer_param), in_hbm(momentum),
            in_hbm(fragment), carried,
        )
    return carried


def shards(
    tokens, norm_gain, inner_weight, cotangent, fragment, outer_param, momentum, lag, threshold
):
    inner_grad = inner_part(tokens, norm_gain, inner_weight, cotangent)
    mixed, new_momentum = fragment_part(fragment, outer_param, momentum, lag, threshold)
    return (inner_grad, mixed, new_momentum)


def solution(mesh):
    placed = (
        P("rep", "fsdp", None),
        P(),
        P("rep", "fsdp", None),
        P("rep", "fsdp", None),
        P("rep", "fsdp", None),
        P("fsdp", None),
        P("fsdp", None),
        P("rep"),
        P(),
    )
    return jax.shard_map(
        shards,
        mesh=mesh,
        in_specs=placed,
        out_specs=(P("rep", "fsdp", None), P("rep", "fsdp", None), P("fsdp", None)),
        check_vma=False,
    )
```

```python
import functools
import math

import jax
import jax.numpy as jnp
from jax import lax
from jax.experimental import pallas as pl
from jax.experimental.pallas import tpu as pltpu
from jax.sharding import PartitionSpec as P


EPS = 1e-05
MU = 0.9
OUTER_LR = 0.7
ALPHA = 0.5
CHUNKS = 2
MARGIN = 16

F32 = jnp.float32
BF16 = jnp.bfloat16


HBM = pl.BlockSpec(memory_space=pltpu.HBM)
VMEM = pl.BlockSpec(memory_space=pltpu.VMEM)
SMEM = pl.BlockSpec(memory_space=pltpu.SMEM)
LANES = 128


def in_hbm(x):
    return pltpu.with_memory_space_constraint(x, pltpu.HBM)


def in_vmem(x):
    return pltpu.with_memory_space_constraint(x, pltpu.VMEM)


def norm_kernel(strip, order_ref, tokens_hbm, gain_hbm, *refs):
    tokens, gain_ref, sems, gain_sem = refs[-4:]
    out_refs = refs[:-4]
    rows, features = tokens.shape
    strips = rows // strip
    groups = out_refs[0].shape[1] // LANES
    step = math.gcd(strip, 16)

    def load(i):
        part = pl.ds(i * strip, strip)
        return pltpu.make_async_copy(tokens_hbm.at[part], tokens.at[part], sems.at[i])

    gain_load = pltpu.make_async_copy(gain_hbm, gain_ref, gain_sem)
    for i in range(strips):
        load(i).start()
    gain_load.start()
    firsts = [pl.multiple_of(order_ref[s] * groups, groups) for s in range(len(out_refs))]
    gain_load.wait()
    for i in range(strips):
        load(i).wait()

        @pl.loop(0, strip // step, unroll=True)
        def _(j):
            part = pl.ds(pl.multiple_of(i * strip + j * step, step), step)
            squares = [jnp.zeros((step, LANES), F32) for _ in range(4)]
            for g in range(features // LANES):
                block = tokens[part, g * LANES : (g + 1) * LANES].astype(F32)
                squares[g % 4] = squares[g % 4] + block * block
            total = (squares[0] + squares[1]) + (squares[2] + squares[3])
            mean = jnp.sum(total, axis=1, keepdims=True) * (1.0 / features)
            scale = jnp.broadcast_to(lax.rsqrt(mean + EPS), (step, LANES))
            for first, out_ref in zip(firsts, out_refs):
                if groups % 8 == 0:
                    gain = gain_ref[pl.ds(first, groups), :].astype(F32)
                else:
                    gain = jnp.concatenate(
                        [gain_ref[pl.ds(first + g, 1), :] for g in range(groups)]
                    )
                for g in range(groups):
                    columns = pl.ds(pl.multiple_of((first + g) * LANES, LANES), LANES)
                    block = tokens[part, columns].astype(F32)
                    out_ref[part, g * LANES : (g + 1) * LANES] = (
                        block * scale * gain[g : g + 1]
                    ).astype(BF16)


def normed_blocks(tokens, norm_gain, order):
    rows, features = tokens.shape
    slots = order.shape[0]
    strip = math.gcd(rows, 32)
    gain = norm_gain.reshape(features // LANES, LANES)
    if features // slots // LANES % 8:
        gain = gain.astype(F32)
    return pl.pallas_call(
        functools.partial(norm_kernel, strip),
        in_specs=[SMEM, HBM, HBM],
        out_specs=[VMEM] * slots,
        out_shape=[jax.ShapeDtypeStruct((rows, features // slots), BF16)] * slots,
        scratch_shapes=[
            pltpu.VMEM((rows, features), BF16),
            pltpu.VMEM(gain.shape, gain.dtype),
            pltpu.SemaphoreType.DMA((rows // strip,)),
            pltpu.SemaphoreType.DMA,
        ],
        cost_estimate=pl.CostEstimate(
            flops=6 * rows * features, bytes_accessed=4 * rows * features, transcendentals=rows
        ),
        compiler_params=pltpu.CompilerParams(vmem_limit_bytes=12 * rows * features),
        name="norm_split",
    )(order, in_hbm(tokens), in_hbm(gain))


def product_kernel(a_ref, b_ref, out_ref):
    out_ref[...] = jnp.dot(a_ref[...], b_ref[...], preferred_element_type=F32).astype(out_ref.dtype)


def product(a, b, dtype):
    rows, depth = a.shape
    width = b.shape[1]
    return pl.pallas_call(
        product_kernel,
        in_specs=[VMEM, VMEM],
        out_specs=VMEM,
        out_shape=jax.ShapeDtypeStruct((rows, width), dtype),
        cost_estimate=pl.CostEstimate(
            flops=2 * rows * depth * width,
            bytes_accessed=2 * (rows * depth + depth * width + rows * width),
            transcendentals=0,
        ),
        compiler_params=pltpu.CompilerParams(
            vmem_limit_bytes=2 * depth * (rows + width) + 16 * rows * width + 2**20
        ),
        name="partial_keys",
    )(in_vmem(a), in_vmem(b))


def gradient_of(normed, dkeys):
    lhs = jnp.concatenate(normed)
    gradient = lax.dot_general(
        lhs, jnp.concatenate(dkeys), (((0,), (0,)), ((), ())), preferred_element_type=F32
    )
    return (gradient * (1.0 / math.sqrt(lhs.shape[0])))[None].astype(BF16)


def inner_part(tokens, norm_gain, inner_weight, cotangent):
    size = lax.axis_size("fsdp")
    me = lax.axis_index("fsdp")
    if size & (size - 1) == 0:
        to = [[i ^ s for i in range(size)] for s in range(size)]
        order = jnp.bitwise_xor(me, jnp.arange(size, dtype=jnp.int32))
    else:
        to = [[(i + s) % size for i in range(size)] for s in range(size)]
        order = lax.rem(me + jnp.arange(size, dtype=jnp.int32), size)

    def send(value, slot):
        return lax.ppermute(value, "fsdp", [(i, to[slot][i]) for i in range(size)])

    def send_back(value, slot):
        return lax.ppermute(value, "fsdp", [(to[slot][i], i) for i in range(size)])

    weight = inner_weight[0]
    blocks = normed_blocks(tokens[0], norm_gain, order)
    normed = [blocks[0]] + [send(blocks[s], s) for s in range(1, size)]
    keys = product(normed[0], weight, F32)
    for s in range(1, size):
        partial_keys = product(normed[s], weight, BF16)
        keys = keys + send_back(partial_keys, s).astype(F32)
    sigmoid_keys = jax.nn.sigmoid(keys)
    slope = sigmoid_keys * (1.0 + keys * (1.0 - sigmoid_keys))
    own = (cotangent[0].astype(F32) * slope).astype(BF16)
    dkeys = [own] + [send(own, s) for s in range(1, size)]
    return gradient_of(normed, dkeys)


def rounded(x):
    return lax.reduce_precision(x, 8, 7).astype(BF16)


def line_sum(term, chips, position, hop):
    half = chips // 2
    for s in range(half - 1):
        term = rounded(term.astype(F32) + hop(term, [(s, s + 1), (chips - 1 - s, chips - 2 - s)]))
    passed = hop(term, [(half - 1, half), (half, half - 1)])
    term = rounded(term.astype(F32) + passed.astype(F32))
    for s in reversed(range(half - 1)):
        passed = hop(term, [(s + 1, s), (chips - 2 - s, chips - 1 - s)])
        term = jnp.where((position == s) | (position == chips - 1 - s), passed, term)
    return term


def outer_kernel(chunk_first, head_ref, *refs):
    totals = refs[:4]
    outer, momentum, frag = refs[4:7]
    mixed_hbm, moment_hbm, mixed, moment, sems = refs[-5:]
    strips, strip, _ = mixed.shape
    half = outer.shape[0] // 2
    rep = lax.axis_index("rep")
    core = lax.rem(rep, 2)
    odd = lax.rem(rep // 2, 2)
    margin = MARGIN
    scale = 1.0 / head_ref[head_ref.shape[0] - margin :, :].astype(F32)

    def start_row(j):
        side = core if j // 2 == 0 else 1 - core
        place = odd if j % 2 == 0 else 1 - odd
        return pl.multiple_of(side * half + chunk_first + place * strip, strip)

    def stores(j):
        rows = pl.ds(start_row(j), strip)
        return (
            pltpu.make_async_copy(mixed.at[j], mixed_hbm.at[0, rows], sems.at[j, 0]),
            pltpu.make_async_copy(moment.at[j], moment_hbm.at[rows], sems.at[j, 1]),
        )

    for j in range(strips):

        @pl.loop(0, strip // margin, unroll=True)
        def _(i):
            part = pl.ds(pl.multiple_of(i * margin, margin), margin)
            rows = pl.ds(pl.multiple_of(start_row(j) + i * margin, margin), margin)
            average = totals[j][part].astype(F32) * scale
            value = outer[rows]
            new_moment = MU * momentum[rows].astype(F32) + average
            new_outer = value - OUTER_LR * (average + MU * new_moment)
            mixed[j, part] = (ALPHA * frag[0, rows].astype(F32) + (1.0 - ALPHA) * new_outer).astype(BF16)
            moment[j, part] = new_moment.astype(BF16)

        for copy in stores(j):
            copy.start()
    for j in range(strips):
        for copy in stores(j):
            copy.wait()


def outer_step(chunk_first, strip, head, totals, outer, momentum, fragment, carried):
    rows, width = outer.shape
    strips = len(totals)
    block = (strips, strip, width)
    return pl.pallas_call(
        functools.partial(outer_kernel, chunk_first),
        in_specs=[VMEM] * (4 + strips) + [HBM] * len(carried),
        out_specs=[HBM, HBM],
        out_shape=[
            jax.ShapeDtypeStruct((1, rows, width), BF16),
            jax.ShapeDtypeStruct((rows, width), BF16),
        ],
        scratch_shapes=[
            pltpu.VMEM(block, BF16),
            pltpu.VMEM(block, BF16),
            pltpu.SemaphoreType.DMA((strips, 2)),
        ],
        input_output_aliases={4 + strips + k: k for k in range(len(carried))},
        cost_estimate=pl.CostEstimate(
            flops=20 * strips * strip * width,
            bytes_accessed=14 * strips * strip * width,
            transcendentals=0,
        ),
        compiler_params=pltpu.CompilerParams(vmem_limit_bytes=6 * strips * strip * width + 2**20),
        name="outer_step",
    )(head, *totals, in_vmem(outer), in_vmem(momentum), in_vmem(fragment), *carried)


def term_kernel(chunk_first, lag_ref, other_lag_ref, threshold_ref, outer_hbm, frag_hbm, other_ref, *refs):
    sent_ref, kept_ref, outer, frag, sems = refs
    part, width = outer.shape[1:]
    half = outer_hbm.shape[0] // 2
    rep = lax.axis_index("rep")
    core = lax.rem(rep, 2)
    odd = lax.rem(rep // 2, 2)

    def start_row(j):
        place = odd if j else 1 - odd
        return pl.multiple_of(core * half + chunk_first + place * part, part)

    def loads(j):
        rows = pl.ds(start_row(j), part)
        return (
            pltpu.make_async_copy(outer_hbm.at[rows], outer.at[j], sems.at[j, 0]),
            pltpu.make_async_copy(frag_hbm.at[0, rows], frag.at[j], sems.at[j, 1]),
        )

    for j in range(2):
        for copy in loads(j):
            copy.start()
    flag = (lag_ref[0] <= threshold_ref[0]).astype(F32)
    other_flag = (other_lag_ref[0] <= threshold_ref[0]).astype(F32)
    step = math.gcd(part, 16)
    for j, out_ref in enumerate((sent_ref, kept_ref)):
        for copy in loads(j):
            copy.wait()

        @pl.loop(0, part // step, unroll=True)
        def _(i):
            rows = pl.ds(pl.multiple_of(i * step, step), step)
            value = outer[j, rows]
            mine = flag * (value - frag[j, rows].astype(F32))
            other_rows = pl.ds(pl.multiple_of(start_row(j) + i * step, step), step)
            theirs = other_flag * (value - other_ref[0, other_rows].astype(F32))
            out_ref[rows, :] = (mine + theirs).astype(out_ref.dtype)

        if out_ref.shape[0] > part:
            margin = out_ref.shape[0] - part
            out_ref[part:, :] = jnp.full((margin, width), flag + other_flag, F32).astype(out_ref.dtype)


def pair_term(chunk_first, part, margin, lag, other_lag, threshold, outer, frag, other):
    width = outer.shape[1]
    return pl.pallas_call(
        functools.partial(term_kernel, chunk_first),
        in_specs=[SMEM] * 3 + [HBM, HBM, VMEM],
        out_specs=[VMEM, VMEM],
        out_shape=[
            jax.ShapeDtypeStruct((part + margin, width), BF16),
            jax.ShapeDtypeStruct((part + margin, width), F32),
        ],
        scratch_shapes=[
            pltpu.VMEM((2, part, width), F32),
            pltpu.VMEM((2, part, width), BF16),
            pltpu.SemaphoreType.DMA((2, 2)),
        ],
        cost_estimate=pl.CostEstimate(
            flops=12 * part * width, bytes_accessed=22 * part * width, transcendentals=0
        ),
        compiler_params=pltpu.CompilerParams(vmem_limit_bytes=32 * (part + margin) * width),
        name="pair_term",
    )(lag, other_lag, threshold, in_hbm(outer), in_hbm(frag), in_vmem(other))


def fragment_part(fragment, outer_param, momentum, lag, threshold):
    size = lax.axis_size("rep")
    rep = lax.axis_index("rep")
    chips = size // 2
    rows = outer_param.shape[0]
    tile = rows // 2 // CHUNKS
    part = tile // 2

    def move(x, pairs):
        return lax.ppermute(x, "rep", pairs)

    def across(x):
        return move(x, [(r, r ^ 1) for r in range(size)])

    def next_chip(x):
        return move(x, [(r, r ^ 2) for r in range(size)])

    other_frag = across(fragment)
    other_lag = across(lag)
    totals = []
    for k in range(CHUNKS):
        sent, kept = pair_term(
            k * tile, part, 0 if k else MARGIN, lag, other_lag, threshold, outer_param, fragment,
            other_frag,
        )
        passed = next_chip(sent)
        value = rounded(kept + passed.astype(F32))

        def hop(x, moves):
            pairs = [(4 * a + r, 4 * b + r) for a, b in moves for r in range(4)]
            return move(x, pairs)

        value = line_sum(value, chips // 2, rep // 4, hop)
        other = next_chip(value)
        far = across(value)
        totals.append((value, other, far, across(other)))
    carried = ()
    for k in range(CHUNKS):
        carried = outer_step(
            k * tile, part, totals[0][0], totals[k], outer_param, momentum, fragment, carried
        )
    return carried


def shards(
    tokens, norm_gain, inner_weight, cotangent, fragment, outer_param, momentum, lag, threshold
):
    inner_grad = inner_part(tokens, norm_gain, inner_weight, cotangent)
    mixed, new_momentum = fragment_part(fragment, outer_param, momentum, lag, threshold)
    return (inner_grad, mixed, new_momentum)


def solution(mesh):
    placed = (
        P("rep", "fsdp", None),
        P(),
        P("rep", "fsdp", None),
        P("rep", "fsdp", None),
        P("rep", "fsdp", None),
        P("fsdp", None),
        P("fsdp", None),
        P("rep"),
        P(),
    )
    return jax.shard_map(
        shards,
        mesh=mesh,
        in_specs=placed,
        out_specs=(P("rep", "fsdp", None), P("rep", "fsdp", None), P("fsdp", None)),
        check_vma=False,
    )
```

```python
import functools
import math

import jax
import jax.numpy as jnp
from jax import lax
from jax.experimental import pallas as pl
from jax.experimental.pallas import tpu as pltpu
from jax.sharding import PartitionSpec as P


EPS = 1e-05
MU = 0.9
OUTER_LR = 0.7
ALPHA = 0.5
SHARES = (1, 2, 1)
MARGIN = 16

F32 = jnp.float32
BF16 = jnp.bfloat16


HBM = pl.BlockSpec(memory_space=pltpu.HBM)
VMEM = pl.BlockSpec(memory_space=pltpu.VMEM)
SMEM = pl.BlockSpec(memory_space=pltpu.SMEM)
LANES = 128


def in_hbm(x):
    return pltpu.with_memory_space_constraint(x, pltpu.HBM)


def in_vmem(x):
    return pltpu.with_memory_space_constraint(x, pltpu.VMEM)


def norm_kernel(strip, order_ref, tokens_hbm, gain_hbm, outer_hbm, frag_hbm, *refs):
    outer_ref, frag_ref, tokens, gain_ref, sems, gain_sem, half_sems = refs[-7:]
    out_refs = refs[:-7]
    rows, features = tokens.shape
    strips = rows // strip
    groups = out_refs[0].shape[1] // LANES
    step = math.gcd(strip, 16)

    def load(i):
        part = pl.ds(i * strip, strip)
        return pltpu.make_async_copy(tokens_hbm.at[part], tokens.at[part], sems.at[i])

    gain_load = pltpu.make_async_copy(gain_hbm, gain_ref, gain_sem)
    load(0).start()
    gain_load.start()
    for i in range(1, strips):
        load(i).start()
    half = outer_ref.shape[0]
    core = lax.rem(lax.axis_index("rep"), 2)
    mine = pl.ds(pl.multiple_of(core * half, half), half)
    half_loads = (
        pltpu.make_async_copy(outer_hbm.at[mine], outer_ref, half_sems.at[0]),
        pltpu.make_async_copy(frag_hbm.at[0, mine], frag_ref, half_sems.at[1]),
    )
    for copy in half_loads:
        copy.start()
    firsts = [pl.multiple_of(order_ref[s] * groups, groups) for s in range(len(out_refs))]
    gain_load.wait()
    for i in range(strips):
        load(i).wait()

        @pl.loop(0, strip // step, unroll=True)
        def _(j):
            part = pl.ds(pl.multiple_of(i * strip + j * step, step), step)
            squares = [jnp.zeros((step, LANES), F32) for _ in range(4)]
            for g in range(features // LANES):
                block = tokens[part, g * LANES : (g + 1) * LANES].astype(F32)
                squares[g % 4] = squares[g % 4] + block * block
            total = (squares[0] + squares[1]) + (squares[2] + squares[3])
            mean = jnp.sum(total, axis=1, keepdims=True) * (1.0 / features)
            scale = jnp.broadcast_to(lax.rsqrt(mean + EPS), (step, LANES))
            for first, out_ref in zip(firsts, out_refs):
                if groups % 8 == 0:
                    gain = gain_ref[pl.ds(first, groups), :].astype(F32)
                else:
                    gain = jnp.concatenate(
                        [gain_ref[pl.ds(first + g, 1), :] for g in range(groups)]
                    )
                for g in range(groups):
                    columns = pl.ds(pl.multiple_of((first + g) * LANES, LANES), LANES)
                    block = tokens[part, columns].astype(F32)
                    out_ref[part, g * LANES : (g + 1) * LANES] = (
                        block * scale * gain[g : g + 1]
                    ).astype(BF16)

    for copy in half_loads:
        copy.wait()


def normed_blocks(tokens, norm_gain, order, outer, fragment):
    half, out_width = outer.shape[0] // 2, outer.shape[1]
    rows, features = tokens.shape
    slots = order.shape[0]
    strip = math.gcd(rows, 32)
    gain = norm_gain.reshape(features // LANES, LANES)
    if features // slots // LANES % 8:
        gain = gain.astype(F32)
    return pl.pallas_call(
        functools.partial(norm_kernel, strip),
        in_specs=[SMEM] + [HBM] * 4,
        out_specs=[VMEM] * (slots + 2),
        out_shape=[jax.ShapeDtypeStruct((rows, features // slots), BF16)] * slots
        + [
            jax.ShapeDtypeStruct((half, out_width), F32),
            jax.ShapeDtypeStruct((half, out_width), BF16),
        ],
        scratch_shapes=[
            pltpu.VMEM((rows, features), BF16),
            pltpu.VMEM(gain.shape, gain.dtype),
            pltpu.SemaphoreType.DMA((rows // strip,)),
            pltpu.SemaphoreType.DMA,
            pltpu.SemaphoreType.DMA((2,)),
        ],
        cost_estimate=pl.CostEstimate(
            flops=6 * rows * features, bytes_accessed=4 * rows * features, transcendentals=rows
        ),
        compiler_params=pltpu.CompilerParams(vmem_limit_bytes=12 * rows * features + 8 * half * out_width),
        name="norm_split",
    )(order, in_hbm(tokens), in_hbm(gain), in_hbm(outer), in_hbm(fragment))


def product_kernel(a_ref, b_ref, out_ref):
    out_ref[...] = jnp.dot(a_ref[...], b_ref[...], preferred_element_type=F32).astype(out_ref.dtype)


def product(a, b, dtype):
    rows, depth = a.shape
    width = b.shape[1]
    return pl.pallas_call(
        product_kernel,
        in_specs=[VMEM, VMEM],
        out_specs=VMEM,
        out_shape=jax.ShapeDtypeStruct((rows, width), dtype),
        cost_estimate=pl.CostEstimate(
            flops=2 * rows * depth * width,
            bytes_accessed=2 * (rows * depth + depth * width + rows * width),
            transcendentals=0,
        ),
        compiler_params=pltpu.CompilerParams(
            vmem_limit_bytes=2 * depth * (rows + width) + 16 * rows * width + 2**20
        ),
        name="partial_keys",
    )(in_vmem(a), in_vmem(b))


def turn_kernel(*refs):
    out_ref = refs[-1]
    for place, ref in enumerate(refs[:-1]):
        rows, features = ref.shape
        block = math.gcd(features, LANES)
        for f in range(0, features, block):
            out_ref[f : f + block, place * rows : (place + 1) * rows] = ref[:, f : f + block].T


def turned(normed):
    rows, features = normed[0].shape
    tokens = rows * len(normed)
    return pl.pallas_call(
        turn_kernel,
        in_specs=[VMEM] * len(normed),
        out_specs=VMEM,
        out_shape=jax.ShapeDtypeStruct((features, tokens), BF16),
        cost_estimate=pl.CostEstimate(
            flops=tokens * features, bytes_accessed=4 * tokens * features, transcendentals=0
        ),
        compiler_params=pltpu.CompilerParams(vmem_limit_bytes=4 * tokens * features + 2**20),
        name="turn",
    )(*(in_vmem(x) for x in normed))


def gradient_kernel(lhs_ref, *refs):
    out_hbm, rhs, out, sems = refs[-4:]
    parts = refs[:-4]
    tokens = lhs_ref.shape[1]
    rows = parts[0].shape[0]
    for place, ref in enumerate(parts):
        rhs[place * rows : (place + 1) * rows, :] = ref[...]
    blocks, block, _ = out.shape
    stores = []
    for j in range(blocks):
        total = jnp.dot(
            lhs_ref[j * block : (j + 1) * block, :], rhs[...], preferred_element_type=F32
        )
        out[j] = (total * (1.0 / math.sqrt(tokens))).astype(BF16)
        stores.append(
            pltpu.make_async_copy(out.at[j], out_hbm.at[0, pl.ds(j * block, block)], sems.at[j])
        )
        stores[j].start()
    for copy in stores:
        copy.wait()


def gradient_of(lhs, dkeys):
    features, tokens = lhs.shape
    _, width = dkeys[0].shape
    block = math.gcd(features, 256)
    return pl.pallas_call(
        gradient_kernel,
        in_specs=[VMEM] * (1 + len(dkeys)),
        out_specs=HBM,
        out_shape=jax.ShapeDtypeStruct((1, features, width), BF16),
        scratch_shapes=[
            pltpu.VMEM((tokens, width), BF16),
            pltpu.VMEM((features // block, block, width), BF16),
            pltpu.SemaphoreType.DMA((features // block,)),
        ],
        cost_estimate=pl.CostEstimate(
            flops=2 * tokens * features * width,
            bytes_accessed=2 * (tokens * (features + width) + features * width),
            transcendentals=0,
        ),
        compiler_params=pltpu.CompilerParams(
            vmem_limit_bytes=2 * width * (tokens + features) + 16 * block * width + 2**21
        ),
        name="key_gradient",
    )(in_vmem(lhs), *(in_vmem(x) for x in dkeys))


def inner_part(tokens, norm_gain, inner_weight, cotangent, outer_param, fragment):
    size = lax.axis_size("fsdp")
    me = lax.axis_index("fsdp")
    if size & (size - 1) == 0:
        to = [[i ^ s for i in range(size)] for s in range(size)]
        order = jnp.bitwise_xor(me, jnp.arange(size, dtype=jnp.int32))
    else:
        to = [[(i + s) % size for i in range(size)] for s in range(size)]
        order = lax.rem(me + jnp.arange(size, dtype=jnp.int32), size)

    def send(value, slot):
        return lax.ppermute(value, "fsdp", [(i, to[slot][i]) for i in range(size)])

    def send_back(value, slot):
        return lax.ppermute(value, "fsdp", [(to[slot][i], i) for i in range(size)])

    weight = inner_weight[0]
    *blocks, outer_half, frag_half = normed_blocks(
        tokens[0], norm_gain, order, outer_param, fragment
    )
    normed = [blocks[0]] + [send(blocks[s], s) for s in range(1, size)]
    keys = product(normed[0], weight, F32)
    for s in range(1, size):
        partial_keys = product(normed[s], weight, BF16)
        keys = keys + send_back(partial_keys, s).astype(F32)
    sigmoid_keys = jax.nn.sigmoid(keys)
    slope = sigmoid_keys * (1.0 + keys * (1.0 - sigmoid_keys))
    own = (cotangent[0].astype(F32) * slope).astype(BF16)
    dkeys = [own] + [send(own, s) for s in range(1, size)]
    lhs = turned(normed)
    return gradient_of(lhs, dkeys), outer_half, frag_half


def rounded(x):
    return lax.reduce_precision(x, 8, 7).astype(BF16)


def line_sum(term, chips, position, hop):
    half = chips // 2
    for s in range(half - 1):
        term = rounded(term.astype(F32) + hop(term, [(s, s + 1), (chips - 1 - s, chips - 2 - s)]))
    passed = hop(term, [(half - 1, half), (half, half - 1)])
    term = rounded(term.astype(F32) + passed.astype(F32))
    for s in reversed(range(half - 1)):
        passed = hop(term, [(s + 1, s), (chips - 2 - s, chips - 1 - s)])
        term = jnp.where((position == s) | (position == chips - 1 - s), passed, term)
    return term


def outer_kernel(chunk_first, head_ref, *refs):
    totals = refs[:4]
    outer, momentum, frag = refs[4:7]
    mixed_hbm, moment_hbm, mixed, moment, sems = refs[-5:]
    strips, strip, _ = mixed.shape
    half = outer.shape[0] // 2
    rep = lax.axis_index("rep")
    core = lax.rem(rep, 2)
    odd = lax.rem(rep // 2, 2)
    margin = MARGIN
    scale = 1.0 / head_ref[head_ref.shape[0] - margin :, :].astype(F32)

    def start_row(j):
        side = core if j // 2 == 0 else 1 - core
        place = odd if j % 2 == 0 else 1 - odd
        return pl.multiple_of(side * half + chunk_first + place * strip, strip)

    def stores(j):
        rows = pl.ds(start_row(j), strip)
        return (
            pltpu.make_async_copy(mixed.at[j], mixed_hbm.at[0, rows], sems.at[j, 0]),
            pltpu.make_async_copy(moment.at[j], moment_hbm.at[rows], sems.at[j, 1]),
        )

    for j in range(strips):

        @pl.loop(0, strip // margin, unroll=True)
        def _(i):
            part = pl.ds(pl.multiple_of(i * margin, margin), margin)
            rows = pl.ds(pl.multiple_of(start_row(j) + i * margin, margin), margin)
            average = totals[j][part].astype(F32) * scale
            value = outer[rows]
            new_moment = MU * momentum[rows].astype(F32) + average
            new_outer = value - OUTER_LR * (average + MU * new_moment)
            mixed[j, part] = (ALPHA * frag[0, rows].astype(F32) + (1.0 - ALPHA) * new_outer).astype(BF16)
            moment[j, part] = new_moment.astype(BF16)

        for copy in stores(j):
            copy.start()
    for j in range(strips):
        for copy in stores(j):
            copy.wait()


def outer_step(chunk_first, strip, head, totals, outer, momentum, fragment, carried):
    rows, width = outer.shape
    strips = len(totals)
    block = (strips, strip, width)
    return pl.pallas_call(
        functools.partial(outer_kernel, chunk_first),
        in_specs=[VMEM] * (4 + strips) + [HBM] * len(carried),
        out_specs=[HBM, HBM],
        out_shape=[
            jax.ShapeDtypeStruct((1, rows, width), BF16),
            jax.ShapeDtypeStruct((rows, width), BF16),
        ],
        scratch_shapes=[
            pltpu.VMEM(block, BF16),
            pltpu.VMEM(block, BF16),
            pltpu.SemaphoreType.DMA((strips, 2)),
        ],
        input_output_aliases={4 + strips + k: k for k in range(len(carried))},
        cost_estimate=pl.CostEstimate(
            flops=20 * strips * strip * width,
            bytes_accessed=14 * strips * strip * width,
            transcendentals=0,
        ),
        compiler_params=pltpu.CompilerParams(vmem_limit_bytes=6 * strips * strip * width + 2**20),
        name="outer_step",
    )(head, *totals, in_vmem(outer), in_vmem(momentum), in_vmem(fragment), *carried)


def term_kernel(chunk_first, part, lag_ref, other_lag_ref, threshold_ref, outer, frag, other, *out_refs):
    half, width = outer.shape
    rep = lax.axis_index("rep")
    core = lax.rem(rep, 2)
    odd = lax.rem(rep // 2, 2)
    flag = (lag_ref[0] <= threshold_ref[0]).astype(F32)
    other_flag = (other_lag_ref[0] <= threshold_ref[0]).astype(F32)
    step = math.gcd(part, 16)
    for j, out_ref in enumerate(out_refs):
        place = odd if j else 1 - odd
        first = pl.multiple_of(chunk_first + place * part, part)

        @pl.loop(0, part // step, unroll=True)
        def _(i):
            rows = pl.ds(pl.multiple_of(first + i * step, step), step)
            other_rows = pl.ds(pl.multiple_of(core * half + first + i * step, step), step)
            value = outer[rows]
            mine = flag * (value - frag[rows].astype(F32))
            theirs = other_flag * (value - other[0, other_rows].astype(F32))
            here = pl.ds(pl.multiple_of(i * step, step), step)
            out_ref[here, :] = (mine + theirs).astype(out_ref.dtype)

        margin = out_ref.shape[0] - part
        if margin > 0:
            count = jnp.full((margin, width), flag + other_flag, F32)
            out_ref[part:, :] = count.astype(out_ref.dtype)


def pair_term(chunk_first, part, margin, lag, other_lag, threshold, outer, frag, other):
    width = outer.shape[1]
    return pl.pallas_call(
        functools.partial(term_kernel, chunk_first, part),
        in_specs=[SMEM] * 3 + [VMEM] * 3,
        out_specs=[VMEM, VMEM],
        out_shape=[
            jax.ShapeDtypeStruct((part + margin, width), BF16),
            jax.ShapeDtypeStruct((part + margin, width), F32),
        ],
        cost_estimate=pl.CostEstimate(
            flops=12 * part * width, bytes_accessed=22 * part * width, transcendentals=0
        ),
        compiler_params=pltpu.CompilerParams(vmem_limit_bytes=16 * part * width + 2**20),
        name="pair_term",
    )(lag, other_lag, threshold, in_vmem(outer), in_vmem(frag), in_vmem(other))


def fragment_part(fragment, outer_param, momentum, lag, threshold, outer_half, frag_half):
    size = lax.axis_size("rep")
    rep = lax.axis_index("rep")
    chips = size // 2
    rows = outer_param.shape[0]
    half = rows // 2
    tiles = [half * share // sum(SHARES) for share in SHARES]
    firsts = [sum(tiles[:k]) for k in range(len(tiles))]

    def move(x, pairs):
        return lax.ppermute(x, "rep", pairs)

    def across(x):
        return move(x, [(r, r ^ 1) for r in range(size)])

    def next_chip(x):
        return move(x, [(r, r ^ 2) for r in range(size)])

    other_frag = across(fragment)
    other_lag = across(lag)
    totals = []
    for k, (first, tile) in enumerate(zip(firsts, tiles)):
        sent, kept = pair_term(
            first, tile // 2, 0 if k else MARGIN, lag, other_lag, threshold, outer_half, frag_half,
            other_frag,
        )
        passed = next_chip(sent)
        value = rounded(kept + passed.astype(F32))

        def hop(x, moves):
            pairs = [(4 * a + r, 4 * b + r) for a, b in moves for r in range(4)]
            return move(x, pairs)

        value = line_sum(value, chips // 2, rep // 4, hop)
        other = next_chip(value)
        far = across(value)
        totals.append((value, other, far, across(other)))
    carried = ()
    for k, (first, tile) in enumerate(zip(firsts, tiles)):
        carried = outer_step(
            first, tile // 2, totals[0][0], totals[k], outer_param, momentum, fragment, carried
        )
    return carried


def shards(
    tokens, norm_gain, inner_weight, cotangent, fragment, outer_param, momentum, lag, threshold
):
    inner_grad, outer_half, frag_half = inner_part(
        tokens, norm_gain, inner_weight, cotangent, outer_param, fragment
    )
    mixed, new_momentum = fragment_part(
        fragment, outer_param, momentum, lag, threshold, outer_half, frag_half
    )
    return (inner_grad, mixed, new_momentum)


def solution(mesh):
    placed = (
        P("rep", "fsdp", None),
        P(),
        P("rep", "fsdp", None),
        P("rep", "fsdp", None),
        P("rep", "fsdp", None),
        P("fsdp", None),
        P("fsdp", None),
        P("rep"),
        P(),
    )
    return jax.shard_map(
        shards,
        mesh=mesh,
        in_specs=placed,
        out_specs=(P("rep", "fsdp", None), P("rep", "fsdp", None), P("fsdp", None)),
        check_vma=False,
    )
```

```python
import functools
import math

import jax
import jax.numpy as jnp
from jax import lax
from jax.experimental import pallas as pl
from jax.experimental.pallas import tpu as pltpu
from jax.sharding import PartitionSpec as P


EPS = 1e-05
MU = 0.9
OUTER_LR = 0.7
ALPHA = 0.5
SHARES = (1, 2, 1)
MARGIN = 16

F32 = jnp.float32
BF16 = jnp.bfloat16


HBM = pl.BlockSpec(memory_space=pltpu.HBM)
VMEM = pl.BlockSpec(memory_space=pltpu.VMEM)
SMEM = pl.BlockSpec(memory_space=pltpu.SMEM)
LANES = 128


def in_hbm(x):
    return pltpu.with_memory_space_constraint(x, pltpu.HBM)


def in_vmem(x):
    return pltpu.with_memory_space_constraint(x, pltpu.VMEM)


def norm_kernel(strip, order_ref, tokens_hbm, gain_hbm, outer_hbm, frag_hbm, *refs):
    outer_ref, frag_ref, tokens, gain_ref, sems, gain_sem, half_sems = refs[-7:]
    out_refs = refs[:-7]
    rows, features = tokens.shape
    strips = rows // strip
    groups = out_refs[0].shape[1] // LANES
    step = math.gcd(strip, 16)

    def load(i):
        part = pl.ds(i * strip, strip)
        return pltpu.make_async_copy(tokens_hbm.at[part], tokens.at[part], sems.at[i])

    gain_load = pltpu.make_async_copy(gain_hbm, gain_ref, gain_sem)
    load(0).start()
    gain_load.start()
    for i in range(1, strips):
        load(i).start()
    half = outer_ref.shape[0]
    core = lax.rem(lax.axis_index("rep"), 2)
    mine = pl.ds(pl.multiple_of(core * half, half), half)
    half_loads = (
        pltpu.make_async_copy(outer_hbm.at[mine], outer_ref, half_sems.at[0]),
        pltpu.make_async_copy(frag_hbm.at[0, mine], frag_ref, half_sems.at[1]),
    )
    for copy in half_loads:
        copy.start()
    firsts = [pl.multiple_of(order_ref[s] * groups, groups) for s in range(len(out_refs))]
    gain_load.wait()
    for i in range(strips):
        load(i).wait()

        @pl.loop(0, strip // step, unroll=True)
        def _(j):
            part = pl.ds(pl.multiple_of(i * strip + j * step, step), step)
            squares = [jnp.zeros((step, LANES), F32) for _ in range(4)]
            for g in range(features // LANES):
                block = tokens[part, g * LANES : (g + 1) * LANES].astype(F32)
                squares[g % 4] = squares[g % 4] + block * block
            total = (squares[0] + squares[1]) + (squares[2] + squares[3])
            mean = jnp.sum(total, axis=1, keepdims=True) * (1.0 / features)
            scale = jnp.broadcast_to(lax.rsqrt(mean + EPS), (step, LANES))
            for first, out_ref in zip(firsts, out_refs):
                if groups % 8 == 0:
                    gain = gain_ref[pl.ds(first, groups), :].astype(F32)
                else:
                    gain = jnp.concatenate(
                        [gain_ref[pl.ds(first + g, 1), :] for g in range(groups)]
                    )
                for g in range(groups):
                    columns = pl.ds(pl.multiple_of((first + g) * LANES, LANES), LANES)
                    block = tokens[part, columns].astype(F32)
                    out_ref[part, g * LANES : (g + 1) * LANES] = (
                        block * scale * gain[g : g + 1]
                    ).astype(BF16)

    for copy in half_loads:
        copy.wait()


def normed_blocks(tokens, norm_gain, order, outer, fragment):
    half, out_width = outer.shape[0] // 2, outer.shape[1]
    rows, features = tokens.shape
    slots = order.shape[0]
    strip = math.gcd(rows, 32)
    gain = norm_gain.reshape(features // LANES, LANES)
    if features // slots // LANES % 8:
        gain = gain.astype(F32)
    return pl.pallas_call(
        functools.partial(norm_kernel, strip),
        in_specs=[SMEM] + [HBM] * 4,
        out_specs=[VMEM] * (slots + 2),
        out_shape=[jax.ShapeDtypeStruct((rows, features // slots), BF16)] * slots
        + [
            jax.ShapeDtypeStruct((half, out_width), F32),
            jax.ShapeDtypeStruct((half, out_width), BF16),
        ],
        scratch_shapes=[
            pltpu.VMEM((rows, features), BF16),
            pltpu.VMEM(gain.shape, gain.dtype),
            pltpu.SemaphoreType.DMA((rows // strip,)),
            pltpu.SemaphoreType.DMA,
            pltpu.SemaphoreType.DMA((2,)),
        ],
        cost_estimate=pl.CostEstimate(
            flops=6 * rows * features, bytes_accessed=4 * rows * features, transcendentals=rows
        ),
        compiler_params=pltpu.CompilerParams(vmem_limit_bytes=12 * rows * features + 8 * half * out_width),
        name="norm_split",
    )(order, in_hbm(tokens), in_hbm(gain), in_hbm(outer), in_hbm(fragment))


def product_kernel(a_ref, b_ref, out_ref):
    out_ref[...] = jnp.dot(a_ref[...], b_ref[...], preferred_element_type=F32).astype(out_ref.dtype)


def product(a, b, dtype):
    rows, depth = a.shape
    width = b.shape[1]
    return pl.pallas_call(
        product_kernel,
        in_specs=[VMEM, VMEM],
        out_specs=VMEM,
        out_shape=jax.ShapeDtypeStruct((rows, width), dtype),
        cost_estimate=pl.CostEstimate(
            flops=2 * rows * depth * width,
            bytes_accessed=2 * (rows * depth + depth * width + rows * width),
            transcendentals=0,
        ),
        compiler_params=pltpu.CompilerParams(
            vmem_limit_bytes=2 * depth * (rows + width) + 16 * rows * width + 2**20
        ),
        name="partial_keys",
    )(in_vmem(a), in_vmem(b))


def turn_kernel(*refs):
    out_ref = refs[-1]
    for place, ref in enumerate(refs[:-1]):
        rows, features = ref.shape
        block = math.gcd(features, LANES)
        for f in range(0, features, block):
            out_ref[f : f + block, place * rows : (place + 1) * rows] = ref[:, f : f + block].T


def turned(normed):
    rows, features = normed[0].shape
    tokens = rows * len(normed)
    return pl.pallas_call(
        turn_kernel,
        in_specs=[VMEM] * len(normed),
        out_specs=VMEM,
        out_shape=jax.ShapeDtypeStruct((features, tokens), BF16),
        cost_estimate=pl.CostEstimate(
            flops=tokens * features, bytes_accessed=4 * tokens * features, transcendentals=0
        ),
        compiler_params=pltpu.CompilerParams(vmem_limit_bytes=4 * tokens * features + 2**20),
        name="turn",
    )(*(in_vmem(x) for x in normed))


def gradient_kernel(lhs_ref, *refs):
    out_hbm, rhs, out, sems = refs[-4:]
    parts = refs[:-4]
    tokens = lhs_ref.shape[1]
    rows = parts[0].shape[0]
    for place, ref in enumerate(parts):
        rhs[place * rows : (place + 1) * rows, :] = ref[...]
    blocks, block, _ = out.shape
    stores = []
    for j in range(blocks):
        total = jnp.dot(
            lhs_ref[j * block : (j + 1) * block, :], rhs[...], preferred_element_type=F32
        )
        out[j] = (total * (1.0 / math.sqrt(tokens))).astype(BF16)
        stores.append(
            pltpu.make_async_copy(out.at[j], out_hbm.at[0, pl.ds(j * block, block)], sems.at[j])
        )
        stores[j].start()
    for copy in stores:
        copy.wait()


def gradient_of(lhs, dkeys):
    features, tokens = lhs.shape
    _, width = dkeys[0].shape
    block = math.gcd(features, 256)
    return pl.pallas_call(
        gradient_kernel,
        in_specs=[VMEM] * (1 + len(dkeys)),
        out_specs=HBM,
        out_shape=jax.ShapeDtypeStruct((1, features, width), BF16),
        scratch_shapes=[
            pltpu.VMEM((tokens, width), BF16),
            pltpu.VMEM((features // block, block, width), BF16),
            pltpu.SemaphoreType.DMA((features // block,)),
        ],
        cost_estimate=pl.CostEstimate(
            flops=2 * tokens * features * width,
            bytes_accessed=2 * (tokens * (features + width) + features * width),
            transcendentals=0,
        ),
        compiler_params=pltpu.CompilerParams(
            vmem_limit_bytes=2 * width * (tokens + features) + 16 * block * width + 2**21
        ),
        name="key_gradient",
    )(in_vmem(lhs), *(in_vmem(x) for x in dkeys))


def inner_part(tokens, norm_gain, inner_weight, cotangent, outer_param, fragment):
    size = lax.axis_size("fsdp")
    me = lax.axis_index("fsdp")
    if size & (size - 1) == 0:
        to = [[i ^ s for i in range(size)] for s in range(size)]
        order = jnp.bitwise_xor(me, jnp.arange(size, dtype=jnp.int32))
    else:
        to = [[(i + s) % size for i in range(size)] for s in range(size)]
        order = lax.rem(me + jnp.arange(size, dtype=jnp.int32), size)

    def send(value, slot):
        return lax.ppermute(value, "fsdp", [(i, to[slot][i]) for i in range(size)])

    def send_back(value, slot):
        return lax.ppermute(value, "fsdp", [(to[slot][i], i) for i in range(size)])

    weight = inner_weight[0]
    *blocks, outer_half, frag_half = normed_blocks(
        tokens[0], norm_gain, order, outer_param, fragment
    )
    normed = [blocks[0]] + [send(blocks[s], s) for s in range(1, size)]
    keys = product(normed[0], weight, F32)
    for s in range(1, size):
        partial_keys = product(normed[s], weight, BF16)
        keys = keys + send_back(partial_keys, s).astype(F32)
    sigmoid_keys = jax.nn.sigmoid(keys)
    slope = sigmoid_keys * (1.0 + keys * (1.0 - sigmoid_keys))
    own = (cotangent[0].astype(F32) * slope).astype(BF16)
    dkeys = [own] + [send(own, s) for s in range(1, size)]
    lhs = turned(normed)
    return gradient_of(lhs, dkeys), outer_half, frag_half


def rounded(x):
    return lax.reduce_precision(x, 8, 7).astype(BF16)


def line_sum(term, chips, position, hop):
    half = chips // 2
    for s in range(half - 1):
        term = rounded(term.astype(F32) + hop(term, [(s, s + 1), (chips - 1 - s, chips - 2 - s)]))
    passed = hop(term, [(half - 1, half), (half, half - 1)])
    term = rounded(term.astype(F32) + passed.astype(F32))
    for s in reversed(range(half - 1)):
        passed = hop(term, [(s + 1, s), (chips - 2 - s, chips - 1 - s)])
        term = jnp.where((position == s) | (position == chips - 1 - s), passed, term)
    return term


def outer_kernel(chunk_first, head_ref, *refs):
    totals = refs[:4]
    outer, momentum, frag = refs[4:7]
    mixed_hbm, moment_hbm, mixed, moment, sems = refs[-5:]
    strips, strip, _ = mixed.shape
    half = outer.shape[0] // 2
    rep = lax.axis_index("rep")
    core = lax.rem(rep, 2)
    odd = lax.rem(rep // 2, 2)
    margin = MARGIN
    scale = 1.0 / head_ref[head_ref.shape[0] - margin :, :].astype(F32)

    def start_row(j):
        side = core if j // 2 == 0 else 1 - core
        place = odd if j % 2 == 0 else 1 - odd
        return pl.multiple_of(side * half + chunk_first + place * strip, strip)

    def stores(j):
        rows = pl.ds(start_row(j), strip)
        return (
            pltpu.make_async_copy(mixed.at[j], mixed_hbm.at[0, rows], sems.at[j, 0]),
            pltpu.make_async_copy(moment.at[j], moment_hbm.at[rows], sems.at[j, 1]),
        )

    for j in range(strips):

        @pl.loop(0, strip // margin, unroll=True)
        def _(i):
            part = pl.ds(pl.multiple_of(i * margin, margin), margin)
            rows = pl.ds(pl.multiple_of(start_row(j) + i * margin, margin), margin)
            average = totals[j][part].astype(F32) * scale
            value = outer[rows]
            new_moment = MU * momentum[rows].astype(F32) + average
            new_outer = value - OUTER_LR * (average + MU * new_moment)
            mixed[j, part] = (ALPHA * frag[0, rows].astype(F32) + (1.0 - ALPHA) * new_outer).astype(BF16)
            moment[j, part] = new_moment.astype(BF16)

        for copy in stores(j):
            copy.start()
    for j in range(strips):
        for copy in stores(j):
            copy.wait()


def outer_step(chunk_first, strip, head, totals, outer, momentum, fragment, carried):
    rows, width = outer.shape
    strips = len(totals)
    block = (strips, strip, width)
    return pl.pallas_call(
        functools.partial(outer_kernel, chunk_first),
        in_specs=[VMEM] * (4 + strips) + [HBM] * len(carried),
        out_specs=[HBM, HBM],
        out_shape=[
            jax.ShapeDtypeStruct((1, rows, width), BF16),
            jax.ShapeDtypeStruct((rows, width), BF16),
        ],
        scratch_shapes=[
            pltpu.VMEM(block, BF16),
            pltpu.VMEM(block, BF16),
            pltpu.SemaphoreType.DMA((strips, 2)),
        ],
        input_output_aliases={4 + strips + k: k for k in range(len(carried))},
        cost_estimate=pl.CostEstimate(
            flops=20 * strips * strip * width,
            bytes_accessed=14 * strips * strip * width,
            transcendentals=0,
        ),
        compiler_params=pltpu.CompilerParams(vmem_limit_bytes=6 * strips * strip * width + 2**20),
        name="outer_step",
    )(head, *totals, in_vmem(outer), in_vmem(momentum), in_vmem(fragment), *carried)


def term_kernel(chunk_first, part, *refs):
    flag_refs, (outer, frag, other), out_refs = refs[:-6], refs[-6:-3], refs[-3:-1]
    half, width = outer.shape
    rep = lax.axis_index("rep")
    core = lax.rem(rep, 2)
    odd = lax.rem(rep // 2, 2)
    flags_out = refs[-1]
    if len(flag_refs) == 1:
        flag, other_flag = flag_refs[0][0:1, 0:1], flag_refs[0][8:9, 0:1]
    else:
        lag_ref, other_lag_ref, threshold_ref = flag_refs
        flag = (lag_ref[0] <= threshold_ref[0]).astype(F32)
        other_flag = (other_lag_ref[0] <= threshold_ref[0]).astype(F32)
        flags_out[0:8, :] = jnp.full((8, LANES), flag, F32)
        flags_out[8:16, :] = jnp.full((8, LANES), other_flag, F32)
    if len(flag_refs) == 1:
        flags_out[...] = flag_refs[0][...]
    step = math.gcd(part, 16)
    for j, out_ref in enumerate(out_refs):
        place = odd if j else 1 - odd
        first = pl.multiple_of(chunk_first + place * part, part)

        @pl.loop(0, part // step, unroll=True)
        def _(i):
            rows = pl.ds(pl.multiple_of(first + i * step, step), step)
            other_rows = pl.ds(pl.multiple_of(core * half + first + i * step, step), step)
            value = outer[rows]
            mine = flag * (value - frag[rows].astype(F32))
            theirs = other_flag * (value - other[0, other_rows].astype(F32))
            here = pl.ds(pl.multiple_of(i * step, step), step)
            out_ref[here, :] = (mine + theirs).astype(out_ref.dtype)

        margin = out_ref.shape[0] - part
        if margin > 0:
            count = jnp.full((margin, width), flag + other_flag, F32)
            out_ref[part:, :] = count.astype(out_ref.dtype)


def pair_term(chunk_first, part, margin, flags, outer, frag, other):
    width = outer.shape[1]
    return pl.pallas_call(
        functools.partial(term_kernel, chunk_first, part),
        in_specs=([SMEM] * 3 if len(flags) == 3 else [VMEM]) + [VMEM] * 3,
        out_specs=[VMEM] * 3,
        out_shape=[
            jax.ShapeDtypeStruct((part + margin, width), BF16),
            jax.ShapeDtypeStruct((part + margin, width), F32),
            jax.ShapeDtypeStruct((16, LANES), F32),
        ],
        cost_estimate=pl.CostEstimate(
            flops=12 * part * width, bytes_accessed=22 * part * width, transcendentals=0
        ),
        compiler_params=pltpu.CompilerParams(vmem_limit_bytes=16 * part * width + 2**20),
        name="pair_term",
    )(*flags, in_vmem(outer), in_vmem(frag), in_vmem(other))


def fragment_part(fragment, outer_param, momentum, lag, threshold, outer_half, frag_half):
    size = lax.axis_size("rep")
    rep = lax.axis_index("rep")
    chips = size // 2
    rows = outer_param.shape[0]
    half = rows // 2
    tiles = [half * share // sum(SHARES) for share in SHARES]
    firsts = [sum(tiles[:k]) for k in range(len(tiles))]

    def move(x, pairs):
        return lax.ppermute(x, "rep", pairs)

    def across(x):
        return move(x, [(r, r ^ 1) for r in range(size)])

    def next_chip(x):
        return move(x, [(r, r ^ 2) for r in range(size)])

    other_frag = across(fragment)
    other_lag = across(lag)
    totals = []
    flags = (lag, other_lag, threshold)
    for k, (first, tile) in enumerate(zip(firsts, tiles)):
        sent, kept, flags = pair_term(
            first, tile // 2, 0 if k else MARGIN, flags, outer_half, frag_half,
            other_frag,
        )
        flags = (in_vmem(flags),)
        passed = next_chip(sent)
        value = rounded(kept + passed.astype(F32))

        def hop(x, moves):
            pairs = [(4 * a + r, 4 * b + r) for a, b in moves for r in range(4)]
            return move(x, pairs)

        value = line_sum(value, chips // 2, rep // 4, hop)
        other = next_chip(value)
        far = across(value)
        totals.append((value, other, far, across(other)))
    carried = ()
    for k, (first, tile) in enumerate(zip(firsts, tiles)):
        carried = outer_step(
            first, tile // 2, totals[0][0], totals[k], outer_param, momentum, fragment, carried
        )
    return carried


def shards(
    tokens, norm_gain, inner_weight, cotangent, fragment, outer_param, momentum, lag, threshold
):
    inner_grad, outer_half, frag_half = inner_part(
        tokens, norm_gain, inner_weight, cotangent, outer_param, fragment
    )
    mixed, new_momentum = fragment_part(
        fragment, outer_param, momentum, lag, threshold, outer_half, frag_half
    )
    return (inner_grad, mixed, new_momentum)


def solution(mesh):
    placed = (
        P("rep", "fsdp", None),
        P(),
        P("rep", "fsdp", None),
        P("rep", "fsdp", None),
        P("rep", "fsdp", None),
        P("fsdp", None),
        P("fsdp", None),
        P("rep"),
        P(),
    )
    return jax.shard_map(
        shards,
        mesh=mesh,
        in_specs=placed,
        out_specs=(P("rep", "fsdp", None), P("rep", "fsdp", None), P("fsdp", None)),
        check_vma=False,
    )
```
